32 devices in a mesh: img: 4 (over x, core), tp: 8 (over z, y).
Axes of the slice: x: 2, y: 2, z: 4, core: 2. Of those that a mesh axis runs over, the one named last changes fastest.
Arguments:
- patch_tokens: bfloat16 [4096, 1024], P(('img', 'tp')), may hold values from -12 to 12
- norm_gain: float32 [1024], replicated, may hold values from 0.1 to 1.9
- norm_bias: float32 [1024], replicated, may hold values from -3 to 3
- up_weight: bfloat16 [1024, 8192], P('img', 'tp'), may hold values from -0.1875 to 0.1875
- up_bias: float32 [8192], P('tp'), may hold values from -3 to 3
- down_weight: bfloat16 [8192, 4096], P('tp', 'img'), may hold values from -0.125 to 0.125
- down_bias: float32 [4096], replicated, may hold values from -3 to 3
Outputs:
- projected: bfloat16 [4096, 4096], P(('img', 'tp'))
The draws below stay inside these ranges and needn't reach their ends.
All inputs are finite; a program needn't handle non-finite values.
Results may differ from the reference program's by a relative error of at most 0.014.
Values may be sent and summed in bfloat16 or wider, within the bound.
A program may use at most 128 MiB of HBM per device.

```python
import jax
import jax.numpy as jnp
from jax import lax

D = 1024
FF = 8192
DOUT = 4096
TOK_DEV = 128
TOKENS = 4096
N_IMG = 4
N_TP = 8


def level_of(own_key, dims, pieces, low, top_value):
    loudness = 1.0
    for axis_at, blocks in pieces:
        draws = jax.random.uniform(jax.random.fold_in(jax.random.fold_in(own_key, 6), axis_at), (blocks,), jnp.float32, low / len(pieces), top_value / len(pieces))
        loudness = loudness * jnp.repeat(jnp.exp(draws), dims[axis_at] // blocks).reshape((-1,) + (1,) * (len(dims) - 1 - axis_at))
    return loudness


def centred(rng, dims, width, reach, pieces=(), held_as=jnp.bfloat16):
    result = width * jax.random.normal(rng, dims, jnp.float32)
    if pieces:
        result = result * level_of(rng, dims, pieces, -0.22, 0.18)
    return jnp.clip(result, -reach, reach).astype(held_as)


def setup_inputs(seed: int = 0) -> dict:
    keys = jax.random.split(jax.random.key(seed), 8)
    patch_tokens = centred(keys[0], (TOKENS, D), 2.0, 12.0, ((0, 32),))
    norm_gain = jnp.clip(1.0 + 0.18 * jax.random.normal(keys[1], (D,), jnp.float32), 0.1, 1.9)
    norm_bias = centred(keys[2], (D,), 0.5, 3.0, (), jnp.float32)
    up_weight = centred(keys[3], (D, FF), D ** -0.5, 0.1875, ((0, 4), (1, 8)))
    up_bias = centred(keys[4], (FF,), 0.5, 3.0, ((0, 8),), jnp.float32)
    down_weight = centred(keys[5], (FF, DOUT), (FF // 4) ** -0.5, 0.125, ((0, 8), (1, 4)))
    down_bias = centred(keys[6], (DOUT,), 0.5, 3.0, (), jnp.float32)
    return dict(patch_tokens=patch_tokens, norm_gain=norm_gain, norm_bias=norm_bias, up_weight=up_weight, up_bias=up_bias, down_weight=down_weight, down_bias=down_bias)


def normalize(rows, norm_gain, norm_bias):
    values = rows.astype(jnp.float32)
    center = lax.optimization_barrier(jnp.mean(values, axis=1, keepdims=True))
    spread = lax.optimization_barrier(jnp.mean((values - center) ** 2, axis=1, keepdims=True))
    return ((values - center) * lax.rsqrt(spread + 1e-05) * norm_gain + norm_bias).astype(jnp.bfloat16)

def reference(patch_tokens, norm_gain, norm_bias, up_weight, up_bias, down_weight, down_bias):
    block_rows = TOK_DEV * N_TP
    group_width = FF // N_TP
    blocks = patch_tokens.reshape(N_IMG, block_rows, D)

    def one_block(rows):
        normed = normalize(rows, norm_gain, norm_bias)
        hidden = jax.nn.gelu(jnp.dot(normed, up_weight, preferred_element_type=jnp.float32) + up_bias).astype(jnp.bfloat16)

        def add_group(group, total):
            start = (group * group_width).astype(jnp.int32)
            cols = lax.dynamic_slice_in_dim(hidden, start, group_width, 1)
            weights = lax.dynamic_slice_in_dim(down_weight, start, group_width, 0)
            partial_value = jnp.dot(cols, weights, preferred_element_type=jnp.float32).astype(jnp.bfloat16)
            partial_value = lax.optimization_barrier(partial_value)
            return total + partial_value.astype(jnp.float32)
        total = lax.fori_loop(0, N_TP, add_group, jnp.zeros((block_rows, DOUT), jnp.float32))
        return (total + down_bias).astype(jnp.bfloat16)
    return lax.map(one_block, blocks).reshape(TOKENS, DOUT)
```

```python
import functools

import jax
import jax.numpy as jnp
from jax import lax
from jax.experimental import pallas as pl
from jax.experimental.pallas import tpu as pltpu
from jax.sharding import PartitionSpec as P

MESH = pl.DeviceIdType.MESH
LANES = 128
UP_STAGES = 2


def kernel(n_img, n_tp, x_ref, gain_ref, nbias_ref, up_ref, ubias_ref, down_ref, dbias_ref, out_ref,
           tok, normed, upf, ubf, hidden, dn, pb, rb,
           tk_s, tk_r, bs_s, bs_r, own_sem, dx_s, dx_r, dm_s, dm_r, r1_s, r1_r, r2_s, r2_r,
           p_s, p_r, rs_s, rs_r):
    cores = 2 if n_img % 2 == 0 else 1
    pair = 2 if n_tp % 2 == 0 else 1
    n_x, n_g = n_img // cores, n_tp // pair
    img, tp = lax.axis_index("img"), lax.axis_index("tp")
    x, c = img // cores, img % cores
    g, m = tp // pair, tp % pair
    rows, width = x_ref.shape
    depth, units = up_ref.shape
    n_chunk = down_ref.shape[1] // LANES
    u_rows = depth // UP_STAGES
    stages = UP_STAGES + n_chunk

    def at_x(k):
        return {"img": lax.rem(x + k, n_x) * cores + c, "tp": tp}

    def at_m(k):
        return {"img": img, "tp": g * pair + lax.rem(m + k, pair)}

    def at_g(k):
        return {"img": img, "tp": lax.rem(g + k, n_g) * pair + m}

    partner = {"img": x * cores + (cores - 1 - c), "tp": tp}
    xs, ms, gs = range(1, n_x), range(1, pair), range(1, n_g)

    def is_up(s):
        return isinstance(s, int) and s < UP_STAGES

    def source(s):
        if is_up(s):
            return up_ref.at[pl.ds(s * u_rows, u_rows), :]
        return down_ref.at[:, pl.ds(pl.multiple_of((s - UP_STAGES) * LANES, LANES), LANES)]

    def block(s, kx, km, core, half=None):
        src = lax.rem(x - kx + n_x, n_x) * cores + core
        src_m = lax.rem(m - km + pair, pair)
        if is_up(s):
            size, lo = u_rows, src * depth + s * u_rows
            if half is not None:
                size, lo = u_rows // 2, lo + half * (u_rows // 2)
            return upf.at[src_m, pl.ds(pl.multiple_of(lo, size), size), :]
        size, lo = units, src_m * units
        if half is not None:
            size, lo = units // 2, lo + half * (units // 2)
        return dn.at[s - UP_STAGES, pl.ds(pl.multiple_of(lo, size), size),
                     pl.ds(pl.multiple_of(src * LANES, LANES), LANES)]

    def copy(src, dst, send, recv, device):
        return pltpu.make_async_remote_copy(
            src_ref=src, dst_ref=dst, send_sem=send, recv_sem=recv,
            device_id=device, device_id_type=MESH)

    def direct_x(s, k, src, dst):
        return copy(src, dst, dx_s.at[s, k], dx_r.at[s, k], at_x(k))

    def direct_m(s, k, src, dst):
        return copy(src, dst, dm_s.at[s, k], dm_r.at[s, k], at_m(k))

    def relay_m(s, kx, km, ref):
        return copy(ref, ref, r1_s.at[s, kx, km], r1_r.at[s, kx, km], at_m(km))

    def relay_x(s, kx, km, ref):
        return copy(ref, ref, r2_s.at[s, kx, km], r2_r.at[s, kx, km], at_x(kx))

    def across(s, kx, km, src, dst):
        return copy(src, dst, p_s.at[s, kx, km], p_r.at[s, kx, km], partner)

    def own_copy(s):
        return pltpu.make_async_copy(source(s), block(s, 0, 0, c), own_sem.at[s])

    def issue(s):
        here, place = source(s), block(s, 0, 0, c)
        for k in xs:
            direct_x(s, k, here, place).start()
        for k in ms:
            direct_m(s, k, here, place).start()
        if cores > 1:
            across(s, 0, 0, here, place).start()
        own_copy(s).start()

    def forward(s):
        for k in xs:
            ref = block(s, k, 0, c)
            direct_x(s, k, ref, ref).wait_recv()
            for km in ms:
                relay_m(s, k, km, block(s, k, 0, c, 0)).start()
            if cores > 1:
                across(s, k, 0, ref, ref).start()
        for km in ms:
            ref = block(s, 0, km, c)
            direct_m(s, km, ref, ref).wait_recv()
            for k in xs:
                relay_x(s, k, km, block(s, 0, km, c, 1)).start()
            if cores > 1:
                across(s, 0, km, ref, ref).start()

    def collect(s):
        for k in xs:
            for km in ms:
                relay_m(s, k, km, block(s, k, km, c, 0)).wait_recv()
                relay_x(s, k, km, block(s, k, km, c, 1)).wait_recv()
                if cores > 1:
                    ref = block(s, k, km, c)
                    across(s, k, km, ref, ref).start()
        own_copy(s).wait()
        if cores > 1:
            for k in range(n_x):
                for km in range(pair):
                    ref = block(s, k, km, cores - 1 - c)
                    across(s, k, km, ref, ref).wait_recv()

    def finish(s):
        for k in xs:
            direct_x(s, k, source(s), source(s)).wait_send()
        for km in ms:
            direct_m(s, km, source(s), source(s)).wait_send()
        for k in xs:
            for km in ms:
                relay_m(s, k, km, block(s, k, 0, c, 0)).wait_send()
                relay_x(s, k, km, block(s, 0, km, c, 1)).wait_send()
        if cores > 1:
            for k in range(n_x):
                for km in range(pair):
                    ref = block(s, k, km, c)
                    across(s, k, km, ref, ref).wait_send()

    def token(k, src, slot):
        return copy(src, tok.at[slot], tk_s.at[k], tk_r.at[k], at_g(k))

    def bias(k, src, slot):
        return copy(src, ubf.at[slot], bs_s.at[k], bs_r.at[k], at_m(k))

    def partial(j, k, src):
        return copy(src, rb.at[j, k - 1], rs_s.at[j, k], rs_r.at[j, k], at_g(k))

    def normalize(values, at):
        values = values.astype(jnp.float32)
        center = jnp.mean(values, axis=1, keepdims=True)
        spread = jnp.mean((values - center) ** 2, axis=1, keepdims=True)
        lines = (values - center) * lax.rsqrt(spread + 1e-05) * gain_ref[...] + nbias_ref[...]
        normed[pl.ds(pl.multiple_of(at * rows, rows), rows), :] = lines.astype(jnp.bfloat16)

    barrier = pltpu.get_barrier_semaphore()
    near = [at_x(k) for k in xs] + [at_m(k) for k in ms] + [at_g(k) for k in gs]
    if cores > 1:
        near.append(partner)
    for device in near:
        pl.semaphore_signal(barrier, inc=1, device_id=device, device_id_type=MESH)
    pl.semaphore_wait(barrier, len(near))

    for k in gs:
        token(k, x_ref, k - 1).start()
    for k in ms:
        bias(k, ubias_ref, k - 1).start()
    issue(0)
    issue(1)
    normalize(x_ref[...], g)

    forward(0)
    issue(2)
    for k in gs:
        token(k, x_ref, k - 1).wait_recv()
        normalize(tok[k - 1], lax.rem(g - k + n_g, n_g))
    for k in ms:
        bias(k, ubias_ref, k - 1).wait_recv()
    forward(1)
    if stages > 3:
        issue(3)
    collect(0)
    forward(2)
    if stages > 4:
        issue(4)
    collect(1)

    tile = 256
    per_m = units // tile

    for km in range(pair):
        place = lax.rem(m - km + pair, pair)
        biases = ubias_ref if km == 0 else ubf.at[km - 1]

        def up_tile(n, carry):
            cols = pl.ds(pl.multiple_of(n * tile, tile), tile)
            summed = jnp.dot(normed[...], upf[place, :, cols], preferred_element_type=jnp.float32)
            wide = pl.ds(pl.multiple_of(place * units + n * tile, tile), tile)
            hidden[:, wide] = jax.nn.gelu(summed + biases[:, cols]).astype(jnp.bfloat16)
            return carry

        lax.fori_loop(0, per_m, up_tile, 0)

    def multiply(j):
        def down_tile(n, carry):
            cols = pl.ds(pl.multiple_of(n * tile, tile), tile)
            value = jnp.dot(hidden[...], dn[j, :, cols], preferred_element_type=jnp.float32)
            pb[j, :, :, cols] = value.reshape(n_g, rows, tile).astype(jnp.bfloat16)
            return carry

        lax.fori_loop(0, n_img * LANES // tile, down_tile, 0)
        for k in gs:
            partial(j, k, pb.at[j, lax.rem(g + k, n_g)]).start()

    def tick(s, carry):
        @pl.when(s < stages)
        def _():
            forward(s)

        @pl.when(s + 2 < stages)
        def _():
            issue(s + 2)

        collect(s - 1)
        multiply(s - 1 - UP_STAGES)
        return carry

    lax.fori_loop(UP_STAGES + 1, stages + 1, tick, 0)

    def reduce(j, carry):
        total = pb[j, g].astype(jnp.float32)
        for k in gs:
            partial(j, k, pb.at[j, 0]).wait_recv()
            total += rb[j, k - 1].astype(jnp.float32)
        for i in range(n_img):
            cols = pl.ds(pl.multiple_of((i * n_chunk + j) * LANES, LANES), LANES)
            part = total[:, i * LANES:(i + 1) * LANES] + dbias_ref[:, cols]
            out_ref[:, cols] = part.astype(jnp.bfloat16)
        for k in gs:
            partial(j, k, pb.at[j, 0]).wait_send()
        return carry

    lax.fori_loop(0, n_chunk, reduce, 0)
    for s in range(UP_STAGES):
        finish(s)

    def finish_tick(s, carry):
        finish(s)
        return carry

    lax.fori_loop(UP_STAGES, stages, finish_tick, 0)
    for k in gs:
        token(k, x_ref, k - 1).wait_send()
    for k in ms:
        bias(k, ubias_ref, k - 1).wait_send()


def solution(mesh):
    n_img, n_tp = mesh.shape["img"], mesh.shape["tp"]
    cores = 2 if n_img % 2 == 0 else 1
    pair = 2 if n_tp % 2 == 0 else 1
    n_x, n_g = n_img // cores, n_tp // pair

    def on_device(x, gain, nbias, up, ubias, down, dbias):
        rows, width = x.shape
        depth, units = up.shape
        n_chunk = down.shape[1] // LANES
        stages = UP_STAGES + n_chunk
        wide = n_img * LANES
        bf16 = jnp.bfloat16
        dma = pltpu.SemaphoreType.DMA
        scratch = [
            pltpu.VMEM((max(n_g - 1, 1), rows, width), bf16),
            pltpu.VMEM((n_g * rows, width), bf16),
            pltpu.VMEM((pair, width, units), bf16),
            pltpu.VMEM((max(pair - 1, 1), 1, units), jnp.float32),
            pltpu.VMEM((n_g * rows, pair * units), bf16),
            pltpu.VMEM((n_chunk, pair * units, wide), bf16),
            pltpu.VMEM((n_chunk, n_g, rows, wide), bf16),
            pltpu.VMEM((n_chunk, max(n_g - 1, 1), rows, wide), bf16),
        ]
        scratch += [dma((n_g,))] * 2 + [dma((pair,))] * 2 + [dma((stages,))]
        scratch += [dma((stages, n_x))] * 2 + [dma((stages, pair))] * 2
        scratch += [dma((stages, n_x, pair))] * 6 + [dma((n_chunk, n_g))] * 2
        return pl.pallas_call(
            functools.partial(kernel, n_img, n_tp),
            out_shape=jax.ShapeDtypeStruct((rows, n_img * down.shape[1]), bf16),
            in_specs=[pl.BlockSpec(memory_space=pltpu.VMEM)] * 7,
            out_specs=pl.BlockSpec(memory_space=pltpu.VMEM),
            scratch_shapes=scratch,
            compiler_params=pltpu.CompilerParams(
                collective_id=0, has_side_effects=True, vmem_limit_bytes=60 * 1024 * 1024),
        )(x, gain.reshape(1, -1), nbias.reshape(1, -1), up, ubias.reshape(1, -1), down,
          dbias.reshape(1, -1))

    return jax.shard_map(
        on_device,
        mesh=mesh,
        in_specs=(P(("img", "tp"), None), P(), P(), P("img", "tp"), P("tp"), P("tp", "img"), P()),
        out_specs=P(("img", "tp"), None),
        check_vma=False,
    )
```

```python
import functools

import jax
import jax.numpy as jnp
from jax import lax
from jax.experimental import pallas as pl
from jax.experimental.pallas import tpu as pltpu
from jax.sharding import PartitionSpec as P

MESH = pl.DeviceIdType.MESH
LANES = 128
UP_STAGES = 2


def kernel(n_img, n_tp, x_ref, gain_ref, nbias_ref, up_ref, ubias_ref, down_ref, dbias_ref, out_ref,
           tok, normed, upf, ubf, hidden, dn, pb, from_low, from_high, sums,
           tk_s, tk_r, bs_s, bs_r, own_sem, dx_s, dx_r, dm_s, dm_r, r1_s, r1_r, r2_s, r2_r,
           p_s, p_r, lo_s, lo_r, hi_s, hi_r):
    cores = 2 if n_img % 2 == 0 else 1
    pair = 2 if n_tp % 2 == 0 else 1
    n_x, n_g = n_img // cores, n_tp // pair
    img, tp = lax.axis_index("img"), lax.axis_index("tp")
    x, c = img // cores, img % cores
    g, m = tp // pair, tp % pair
    rows, width = x_ref.shape
    depth, units = up_ref.shape
    n_chunk = down_ref.shape[1] // LANES
    u_rows = depth // UP_STAGES
    stages = UP_STAGES + n_chunk

    def at_x(k):
        return {"img": lax.rem(x + k, n_x) * cores + c, "tp": tp}

    def at_m(k):
        return {"img": img, "tp": g * pair + lax.rem(m + k, pair)}

    def at_g(k):
        return {"img": img, "tp": lax.rem(g + k, n_g) * pair + m}

    partner = {"img": x * cores + (cores - 1 - c), "tp": tp}
    xs, ms, gs = range(1, n_x), range(1, pair), range(1, n_g)

    def is_up(s):
        return isinstance(s, int) and s < UP_STAGES

    def source(s):
        if is_up(s):
            return up_ref.at[pl.ds(s * u_rows, u_rows), :]
        return down_ref.at[:, pl.ds(pl.multiple_of((s - UP_STAGES) * LANES, LANES), LANES)]

    def block(s, kx, km, core, half=None):
        src = lax.rem(x - kx + n_x, n_x) * cores + core
        src_m = lax.rem(m - km + pair, pair)
        if is_up(s):
            size, lo = u_rows, src * depth + s * u_rows
            if half is not None:
                size, lo = u_rows // 2, lo + half * (u_rows // 2)
            return upf.at[src_m, pl.ds(pl.multiple_of(lo, size), size), :]
        size, lo = units, src_m * units
        if half is not None:
            size, lo = units // 2, lo + half * (units // 2)
        return dn.at[s - UP_STAGES, pl.ds(pl.multiple_of(lo, size), size),
                     pl.ds(pl.multiple_of(src * LANES, LANES), LANES)]

    def copy(src, dst, send, recv, device):
        return pltpu.make_async_remote_copy(
            src_ref=src, dst_ref=dst, send_sem=send, recv_sem=recv,
            device_id=device, device_id_type=MESH)

    def direct_x(s, k, src, dst):
        return copy(src, dst, dx_s.at[s, k], dx_r.at[s, k], at_x(k))

    def direct_m(s, k, src, dst):
        return copy(src, dst, dm_s.at[s, k], dm_r.at[s, k], at_m(k))

    def relay_m(s, kx, km, ref):
        return copy(ref, ref, r1_s.at[s, kx, km], r1_r.at[s, kx, km], at_m(km))

    def relay_x(s, kx, km, ref):
        return copy(ref, ref, r2_s.at[s, kx, km], r2_r.at[s, kx, km], at_x(kx))

    def across(s, kx, km, src, dst):
        return copy(src, dst, p_s.at[s, kx, km], p_r.at[s, kx, km], partner)

    def own_copy(s):
        return pltpu.make_async_copy(source(s), block(s, 0, 0, c), own_sem.at[s])

    def issue(s):
        here, place = source(s), block(s, 0, 0, c)
        for k in xs:
            direct_x(s, k, here, place).start()
        for k in ms:
            direct_m(s, k, here, place).start()
        if cores > 1:
            across(s, 0, 0, here, place).start()
        own_copy(s).start()

    def forward(s):
        for k in xs:
            ref = block(s, k, 0, c)
            direct_x(s, k, ref, ref).wait_recv()
            for km in ms:
                relay_m(s, k, km, block(s, k, 0, c, 0)).start()
            if cores > 1:
                across(s, k, 0, ref, ref).start()
        for km in ms:
            ref = block(s, 0, km, c)
            direct_m(s, km, ref, ref).wait_recv()
            for k in xs:
                relay_x(s, k, km, block(s, 0, km, c, 1)).start()
            if cores > 1:
                across(s, 0, km, ref, ref).start()

    def collect(s):
        for k in xs:
            for km in ms:
                relay_m(s, k, km, block(s, k, km, c, 0)).wait_recv()
                relay_x(s, k, km, block(s, k, km, c, 1)).wait_recv()
                if cores > 1:
                    ref = block(s, k, km, c)
                    across(s, k, km, ref, ref).start()
        own_copy(s).wait()
        if cores > 1:
            for k in range(n_x):
                for km in range(pair):
                    ref = block(s, k, km, cores - 1 - c)
                    across(s, k, km, ref, ref).wait_recv()

    def finish(s):
        for k in xs:
            direct_x(s, k, source(s), source(s)).wait_send()
        for km in ms:
            direct_m(s, km, source(s), source(s)).wait_send()
        for k in xs:
            for km in ms:
                relay_m(s, k, km, block(s, k, 0, c, 0)).wait_send()
                relay_x(s, k, km, block(s, 0, km, c, 1)).wait_send()
        if cores > 1:
            for k in range(n_x):
                for km in range(pair):
                    ref = block(s, k, km, c)
                    across(s, k, km, ref, ref).wait_send()

    def token(k, src, slot):
        return copy(src, tok.at[slot], tk_s.at[k], tk_r.at[k], at_g(k))

    def bias(k, src, slot):
        return copy(src, ubf.at[slot], bs_s.at[k], bs_r.at[k], at_m(k))

    def upward(j, d):
        return copy(pb.at[j, d], from_low.at[j, d], lo_s.at[j, d], lo_r.at[j, d], at_g(1))

    def downward(j, d):
        return copy(pb.at[j, d], from_high.at[j, d], hi_s.at[j, d], hi_r.at[j, d], at_g(n_g - 1))

    def normalize(values, at):
        values = values.astype(jnp.float32)
        center = jnp.mean(values, axis=1, keepdims=True)
        spread = jnp.mean((values - center) ** 2, axis=1, keepdims=True)
        lines = (values - center) * lax.rsqrt(spread + 1e-05) * gain_ref[...] + nbias_ref[...]
        normed[pl.ds(pl.multiple_of(at * rows, rows), rows), :] = lines.astype(jnp.bfloat16)

    barrier = pltpu.get_barrier_semaphore()
    near = [at_x(k) for k in xs] + [at_m(k) for k in ms] + [at_g(k) for k in gs]
    if cores > 1:
        near.append(partner)
    for device in near:
        pl.semaphore_signal(barrier, inc=1, device_id=device, device_id_type=MESH)
    pl.semaphore_wait(barrier, len(near))

    for k in gs:
        token(k, x_ref, k - 1).start()
    for k in ms:
        bias(k, ubias_ref, k - 1).start()
    issue(0)
    issue(1)
    normalize(x_ref[...], g)

    forward(0)
    issue(2)
    for k in gs:
        token(k, x_ref, k - 1).wait_recv()
        normalize(tok[k - 1], lax.rem(g - k + n_g, n_g))
    for k in ms:
        bias(k, ubias_ref, k - 1).wait_recv()
    forward(1)
    if stages > 3:
        issue(3)
    collect(0)
    forward(2)
    if stages > 4:
        issue(4)
    collect(1)

    tile = 256
    per_m = units // tile

    for km in range(pair):
        place = lax.rem(m - km + pair, pair)
        biases = ubias_ref if km == 0 else ubf.at[km - 1]

        def up_tile(n, carry):
            cols = pl.ds(pl.multiple_of(n * tile, tile), tile)
            summed = jnp.dot(normed[...], upf[place, :, cols], preferred_element_type=jnp.float32)
            wide = pl.ds(pl.multiple_of(place * units + n * tile, tile), tile)
            hidden[:, wide] = jax.nn.gelu(summed + biases[:, cols]).astype(jnp.bfloat16)
            return carry

        lax.fori_loop(0, per_m, up_tile, 0)

    def multiply(j):
        def down_tile(n, carry):
            cols = pl.ds(pl.multiple_of(n * tile, tile), tile)
            value = jnp.dot(hidden[...], dn[j, :, cols], preferred_element_type=jnp.float32)
            pb[j, :, :, cols] = value.reshape(n_g, rows, tile).astype(jnp.bfloat16)
            return carry

        lax.fori_loop(0, n_img * LANES // tile, down_tile, 0)

    def pass_on(step):
        j_up, j_down = step - g, step - (n_g - 1 - g)
        go_up = (g < n_g - 1) & (j_up >= 0) & (j_up < n_chunk)
        go_down = (g > 0) & (j_down >= 0) & (j_down < n_chunk)

        def accumulate(j, d, copies, arrived):
            copies(j, d).wait_recv()
            pb[j, d] = (pb[j, d].astype(jnp.float32) + arrived[j, d].astype(jnp.float32)).astype(jnp.bfloat16)

        for d in reversed(range(1, n_g)):
            @pl.when(go_up & (g > 0) & (g < d))
            def _():
                accumulate(j_up, d, upward, from_low)
        for d in range(n_g - 1):
            @pl.when(go_down & (g < n_g - 1) & (g > d))
            def _():
                accumulate(j_down, d, downward, from_high)
        for d in reversed(range(1, n_g)):
            @pl.when(go_up & (g < d))
            def _():
                upward(j_up, d).start()
        for d in range(n_g - 1):
            @pl.when(go_down & (g > d))
            def _():
                downward(j_down, d).start()

    def tick(s, carry):
        @pl.when(s < stages)
        def _():
            forward(s)

        @pl.when(s + 2 < stages)
        def _():
            issue(s + 2)

        step = s - 1 - UP_STAGES
        collect(s - 1)
        multiply(step)
        pass_on(step)

        @pl.when(step >= n_g)
        def _():
            reduce(step - n_g)
        return carry

    def reduce(j):
        total = pb[j, g].astype(jnp.float32)
        for i in range(n_img):
            cols = pl.ds(pl.multiple_of((i * n_chunk + j) * LANES, LANES), LANES)
            piece = slice(i * LANES, (i + 1) * LANES)
            sums[:, piece] = total[:, piece] + dbias_ref[:, cols]
        for first, copies, arrived in ((g > 0, upward, from_low), (g < n_g - 1, downward, from_high)):
            @pl.when(first)
            def _():
                copies(j, g).wait_recv()
                sums[...] += arrived[j, g].astype(jnp.float32)
        for i in range(n_img):
            cols = pl.ds(pl.multiple_of((i * n_chunk + j) * LANES, LANES), LANES)
            out_ref[:, cols] = sums[:, i * LANES:(i + 1) * LANES].astype(jnp.bfloat16)

    def drain(step, carry):
        pass_on(step)
        return carry

    def reduce_tick(j, carry):
        reduce(j)
        return carry

    def sent(j, carry):
        for d in range(n_g):
            @pl.when(g < d)
            def _():
                upward(j, d).wait_send()

            @pl.when(g > d)
            def _():
                downward(j, d).wait_send()
        return carry

    lax.fori_loop(UP_STAGES + 1, stages + 1, tick, 0)
    lax.fori_loop(n_chunk, n_chunk + n_g - 2, drain, 0)
    lax.fori_loop(max(n_chunk - n_g, 0), n_chunk, reduce_tick, 0)
    lax.fori_loop(0, n_chunk, sent, 0)
    for s in range(UP_STAGES):
        finish(s)

    def finish_tick(s, carry):
        finish(s)
        return carry

    lax.fori_loop(UP_STAGES, stages, finish_tick, 0)
    for k in gs:
        token(k, x_ref, k - 1).wait_send()
    for k in ms:
        bias(k, ubias_ref, k - 1).wait_send()


def solution(mesh):
    n_img, n_tp = mesh.shape["img"], mesh.shape["tp"]
    cores = 2 if n_img % 2 == 0 else 1
    pair = 2 if n_tp % 2 == 0 else 1
    n_x, n_g = n_img // cores, n_tp // pair

    def on_device(x, gain, nbias, up, ubias, down, dbias):
        rows, width = x.shape
        depth, units = up.shape
        n_chunk = down.shape[1] // LANES
        stages = UP_STAGES + n_chunk
        wide = n_img * LANES
        bf16 = jnp.bfloat16
        dma = pltpu.SemaphoreType.DMA
        scratch = [
            pltpu.VMEM((max(n_g - 1, 1), rows, width), bf16),
            pltpu.VMEM((n_g * rows, width), bf16),
            pltpu.VMEM((pair, width, units), bf16),
            pltpu.VMEM((max(pair - 1, 1), 1, units), jnp.float32),
            pltpu.VMEM((n_g * rows, pair * units), bf16),
            pltpu.VMEM((n_chunk, pair * units, wide), bf16),
            pltpu.VMEM((n_chunk, n_g, rows, wide), bf16),
            pltpu.VMEM((n_chunk, n_g, rows, wide), bf16),
            pltpu.VMEM((n_chunk, n_g, rows, wide), bf16),
            pltpu.VMEM((rows, wide), jnp.float32),
        ]
        scratch += [dma((n_g,))] * 2 + [dma((pair,))] * 2 + [dma((stages,))]
        scratch += [dma((stages, n_x))] * 2 + [dma((stages, pair))] * 2
        scratch += [dma((stages, n_x, pair))] * 6 + [dma((n_chunk, n_g))] * 4
        return pl.pallas_call(
            functools.partial(kernel, n_img, n_tp),
            out_shape=jax.ShapeDtypeStruct((rows, n_img * down.shape[1]), bf16),
            in_specs=[pl.BlockSpec(memory_space=pltpu.VMEM)] * 7,
            out_specs=pl.BlockSpec(memory_space=pltpu.VMEM),
            scratch_shapes=scratch,
            compiler_params=pltpu.CompilerParams(
                collective_id=0, has_side_effects=True, vmem_limit_bytes=60 * 1024 * 1024),
        )(x, gain.reshape(1, -1), nbias.reshape(1, -1), up, ubias.reshape(1, -1), down,
          dbias.reshape(1, -1))

    return jax.shard_map(
        on_device,
        mesh=mesh,
        in_specs=(P(("img", "tp"), None), P(), P(), P("img", "tp"), P("tp"), P("tp", "img"), P()),
        out_specs=P(("img", "tp"), None),
        check_vma=False,
    )
```

```python
import functools

import jax
import jax.numpy as jnp
from jax import lax
from jax.experimental import pallas as pl
from jax.experimental.pallas import tpu as pltpu
from jax.sharding import PartitionSpec as P

MESH = pl.DeviceIdType.MESH
LANES = 128
UP_STAGES = 2


def kernel(n_img, n_tp, x_ref, gain_ref, nbias_ref, up_ref, ubias_ref, down_ref, dbias_ref, out_ref,
           tok, normed, upf, ubf, hidden, dn, pb, from_low, from_high, sums,
           tk_s, tk_r, bs_s, bs_r, own_sem, dx_s, dx_r, dm_s, dm_r, r1_s, r1_r, r2_s, r2_r,
           p_s, p_r, lo_s, lo_r, hi_s, hi_r):
    cores = 2 if n_img % 2 == 0 else 1
    pair = 2 if n_tp % 2 == 0 else 1
    n_x, n_g = n_img // cores, n_tp // pair
    img, tp = lax.axis_index("img"), lax.axis_index("tp")
    x, c = img // cores, img % cores
    g, m = tp // pair, tp % pair
    rows, width = x_ref.shape
    depth, units = up_ref.shape
    n_chunk = down_ref.shape[1] // LANES
    u_rows = depth // UP_STAGES
    stages = UP_STAGES + n_chunk

    def at_x(k):
        return {"img": lax.rem(x + k, n_x) * cores + c, "tp": tp}

    def at_m(k):
        return {"img": img, "tp": g * pair + lax.rem(m + k, pair)}

    def at_g(k):
        return {"img": img, "tp": lax.rem(g + k, n_g) * pair + m}

    partner = {"img": x * cores + (cores - 1 - c), "tp": tp}
    xs, ms, gs = range(1, n_x), range(1, pair), range(1, n_g)

    def is_up(s):
        return isinstance(s, int) and s < UP_STAGES

    def source(s):
        if is_up(s):
            return up_ref.at[pl.ds(s * u_rows, u_rows), :]
        return down_ref.at[:, pl.ds(pl.multiple_of((s - UP_STAGES) * LANES, LANES), LANES)]

    def block(s, kx, km, core, half=None):
        src = lax.rem(x - kx + n_x, n_x) * cores + core
        src_m = lax.rem(m - km + pair, pair)
        if is_up(s):
            size, lo = u_rows, src * depth + s * u_rows
            if half is not None:
                size, lo = u_rows // 2, lo + half * (u_rows // 2)
            return upf.at[src_m, pl.ds(pl.multiple_of(lo, size), size), :]
        size, lo = units, src_m * units
        if half is not None:
            size, lo = units // 2, lo + half * (units // 2)
        return dn.at[s - UP_STAGES, pl.ds(pl.multiple_of(lo, size), size),
                     pl.ds(pl.multiple_of(src * LANES, LANES), LANES)]

    def copy(src, dst, send, recv, device):
        return pltpu.make_async_remote_copy(
            src_ref=src, dst_ref=dst, send_sem=send, recv_sem=recv,
            device_id=device, device_id_type=MESH)

    def direct_x(s, k, src, dst):
        return copy(src, dst, dx_s.at[s, k], dx_r.at[s, k], at_x(k))

    def direct_m(s, k, src, dst):
        return copy(src, dst, dm_s.at[s, k], dm_r.at[s, k], at_m(k))

    def relay_m(s, kx, km, ref):
        return copy(ref, ref, r1_s.at[s, kx, km], r1_r.at[s, kx, km], at_m(km))

    def relay_x(s, kx, km, ref):
        return copy(ref, ref, r2_s.at[s, kx, km], r2_r.at[s, kx, km], at_x(kx))

    def across(s, kx, km, src, dst):
        return copy(src, dst, p_s.at[s, kx, km], p_r.at[s, kx, km], partner)

    def own_copy(s):
        return pltpu.make_async_copy(source(s), block(s, 0, 0, c), own_sem.at[s])

    def issue(s):
        here, place = source(s), block(s, 0, 0, c)
        for k in xs:
            direct_x(s, k, here, place).start()
        for k in ms:
            direct_m(s, k, here, place).start()
        if cores > 1:
            across(s, 0, 0, here, place).start()
        own_copy(s).start()

    def forward(s):
        for k in xs:
            ref = block(s, k, 0, c)
            direct_x(s, k, ref, ref).wait_recv()
            for km in ms:
                relay_m(s, k, km, block(s, k, 0, c, 0)).start()
            if cores > 1:
                across(s, k, 0, ref, ref).start()
        for km in ms:
            ref = block(s, 0, km, c)
            direct_m(s, km, ref, ref).wait_recv()
            for k in xs:
                relay_x(s, k, km, block(s, 0, km, c, 1)).start()
            if cores > 1:
                across(s, 0, km, ref, ref).start()

    def collect(s):
        for k in xs:
            for km in ms:
                relay_m(s, k, km, block(s, k, km, c, 0)).wait_recv()
                relay_x(s, k, km, block(s, k, km, c, 1)).wait_recv()
                if cores > 1:
                    ref = block(s, k, km, c)
                    across(s, k, km, ref, ref).start()
        own_copy(s).wait()
        if cores > 1:
            for k in range(n_x):
                for km in range(pair):
                    ref = block(s, k, km, cores - 1 - c)
                    across(s, k, km, ref, ref).wait_recv()

    def finish(s):
        for k in xs:
            direct_x(s, k, source(s), source(s)).wait_send()
        for km in ms:
            direct_m(s, km, source(s), source(s)).wait_send()
        for k in xs:
            for km in ms:
                relay_m(s, k, km, block(s, k, 0, c, 0)).wait_send()
                relay_x(s, k, km, block(s, 0, km, c, 1)).wait_send()
        if cores > 1:
            for k in range(n_x):
                for km in range(pair):
                    ref = block(s, k, km, c)
                    across(s, k, km, ref, ref).wait_send()

    def token(k, src, slot):
        return copy(src, tok.at[slot], tk_s.at[k], tk_r.at[k], at_g(k))

    def bias(k, src, slot):
        return copy(src, ubf.at[slot], bs_s.at[k], bs_r.at[k], at_m(k))

    def upward(j, d):
        return copy(pb.at[j, d], from_low.at[j, d], lo_s.at[j, d], lo_r.at[j, d], at_g(1))

    def downward(j, d):
        return copy(pb.at[j, d], from_high.at[j, d], hi_s.at[j, d], hi_r.at[j, d], at_g(n_g - 1))

    def normalize(values, at):
        values = values.astype(jnp.float32)
        center = jnp.mean(values, axis=1, keepdims=True)
        spread = jnp.mean((values - center) ** 2, axis=1, keepdims=True)
        lines = (values - center) * lax.rsqrt(spread + 1e-05) * gain_ref[...] + nbias_ref[...]
        normed[pl.ds(pl.multiple_of(at * rows, rows), rows), :] = lines.astype(jnp.bfloat16)

    barrier = pltpu.get_barrier_semaphore()
    near = [at_x(k) for k in xs] + [at_m(k) for k in ms] + [at_g(k) for k in gs]
    if cores > 1:
        near.append(partner)
    for device in near:
        pl.semaphore_signal(barrier, inc=1, device_id=device, device_id_type=MESH)
    pl.semaphore_wait(barrier, len(near))

    for k in gs:
        token(k, x_ref, k - 1).start()
    for k in ms:
        bias(k, ubias_ref, k - 1).start()
    issue(0)
    issue(1)
    normalize(x_ref[...], g)

    forward(0)
    issue(2)
    forward(1)
    if stages > 3:
        issue(3)
    collect(0)
    forward(2)
    if stages > 4:
        issue(4)
    for k in gs:
        token(k, x_ref, k - 1).wait_recv()
        normalize(tok[k - 1], lax.rem(g - k + n_g, n_g))
    for k in ms:
        bias(k, ubias_ref, k - 1).wait_recv()
    collect(1)

    tile = 256
    per_m = units // tile

    for km in range(pair):
        place = lax.rem(m - km + pair, pair)
        biases = ubias_ref if km == 0 else ubf.at[km - 1]

        def up_tile(n, carry):
            cols = pl.ds(pl.multiple_of(n * tile, tile), tile)
            summed = jnp.dot(normed[...], upf[place, :, cols], preferred_element_type=jnp.float32)
            wide = pl.ds(pl.multiple_of(place * units + n * tile, tile), tile)
            hidden[:, wide] = jax.nn.gelu(summed + biases[:, cols]).astype(jnp.bfloat16)
            return carry

        lax.fori_loop(0, per_m, up_tile, 0)

    def multiply(j):
        def down_tile(n, carry):
            cols = pl.ds(pl.multiple_of(n * tile, tile), tile)
            value = jnp.dot(hidden[...], dn[j, :, cols], preferred_element_type=jnp.float32)
            pb[j, :, :, cols] = value.reshape(n_g, rows, tile).astype(jnp.bfloat16)
            return carry

        lax.fori_loop(0, n_img * LANES // tile, down_tile, 0)

    def pass_on(step):
        j_up, j_down = step - g, step - (n_g - 1 - g)
        go_up = (g < n_g - 1) & (j_up >= 0) & (j_up < n_chunk)
        go_down = (g > 0) & (j_down >= 0) & (j_down < n_chunk)

        def accumulate(j, d, copies, arrived):
            copies(j, d).wait_recv()
            pb[j, d] = (pb[j, d].astype(jnp.float32) + arrived[j, d].astype(jnp.float32)).astype(jnp.bfloat16)

        for k in range(n_g - 1):
            high, low = n_g - 1 - k, k

            @pl.when(go_up & (g > 0) & (g < high))
            def _():
                accumulate(j_up, high, upward, from_low)

            @pl.when(go_down & (g < n_g - 1) & (g > low))
            def _():
                accumulate(j_down, low, downward, from_high)

            @pl.when(go_up & (g < high))
            def _():
                upward(j_up, high).start()

            @pl.when(go_down & (g > low))
            def _():
                downward(j_down, low).start()

    def tick(s, carry):
        @pl.when(s < stages)
        def _():
            forward(s)

        @pl.when(s + 2 < stages)
        def _():
            issue(s + 2)

        step = s - 1 - UP_STAGES
        collect(s - 1)
        multiply(step)
        pass_on(step)

        @pl.when(step >= n_g)
        def _():
            reduce(step - n_g)
        return carry

    def reduce(j):
        total = pb[j, g].astype(jnp.float32)
        for i in range(n_img):
            cols = pl.ds(pl.multiple_of((i * n_chunk + j) * LANES, LANES), LANES)
            piece = slice(i * LANES, (i + 1) * LANES)
            sums[:, piece] = total[:, piece] + dbias_ref[:, cols]
        for first, copies, arrived in ((g > 0, upward, from_low), (g < n_g - 1, downward, from_high)):
            @pl.when(first)
            def _():
                copies(j, g).wait_recv()
                sums[...] += arrived[j, g].astype(jnp.float32)
        for i in range(n_img):
            cols = pl.ds(pl.multiple_of((i * n_chunk + j) * LANES, LANES), LANES)
            out_ref[:, cols] = sums[:, i * LANES:(i + 1) * LANES].astype(jnp.bfloat16)

    def drain(step, carry):
        pass_on(step)
        return carry

    def reduce_tick(j, carry):
        reduce(j)
        return carry

    def sent(j, carry):
        for d in range(n_g):
            @pl.when(g < d)
            def _():
                upward(j, d).wait_send()

            @pl.when(g > d)
            def _():
                downward(j, d).wait_send()
        return carry

    lax.fori_loop(UP_STAGES + 1, stages + 1, tick, 0)
    lax.fori_loop(n_chunk, n_chunk + n_g - 2, drain, 0)
    lax.fori_loop(max(n_chunk - n_g, 0), n_chunk, reduce_tick, 0)
    lax.fori_loop(0, n_chunk, sent, 0)
    for s in range(UP_STAGES):
        finish(s)

    def finish_tick(s, carry):
        finish(s)
        return carry

    lax.fori_loop(UP_STAGES, stages, finish_tick, 0)
    for k in gs:
        token(k, x_ref, k - 1).wait_send()
    for k in ms:
        bias(k, ubias_ref, k - 1).wait_send()


def solution(mesh):
    n_img, n_tp = mesh.shape["img"], mesh.shape["tp"]
    cores = 2 if n_img % 2 == 0 else 1
    pair = 2 if n_tp % 2 == 0 else 1
    n_x, n_g = n_img // cores, n_tp // pair

    def on_device(x, gain, nbias, up, ubias, down, dbias):
        rows, width = x.shape
        depth, units = up.shape
        n_chunk = down.shape[1] // LANES
        stages = UP_STAGES + n_chunk
        wide = n_img * LANES
        bf16 = jnp.bfloat16
        dma = pltpu.SemaphoreType.DMA
        scratch = [
            pltpu.VMEM((max(n_g - 1, 1), rows, width), bf16),
            pltpu.VMEM((n_g * rows, width), bf16),
            pltpu.VMEM((pair, width, units), bf16),
            pltpu.VMEM((max(pair - 1, 1), 1, units), jnp.float32),
            pltpu.VMEM((n_g * rows, pair * units), bf16),
            pltpu.VMEM((n_chunk, pair * units, wide), bf16),
            pltpu.VMEM((n_chunk, n_g, rows, wide), bf16),
            pltpu.VMEM((n_chunk, n_g, rows, wide), bf16),
            pltpu.VMEM((n_chunk, n_g, rows, wide), bf16),
            pltpu.VMEM((rows, wide), jnp.float32),
        ]
        scratch += [dma((n_g,))] * 2 + [dma((pair,))] * 2 + [dma((stages,))]
        scratch += [dma((stages, n_x))] * 2 + [dma((stages, pair))] * 2
        scratch += [dma((stages, n_x, pair))] * 6 + [dma((n_chunk, n_g))] * 4
        return pl.pallas_call(
            functools.partial(kernel, n_img, n_tp),
            out_shape=jax.ShapeDtypeStruct((rows, n_img * down.shape[1]), bf16),
            in_specs=[pl.BlockSpec(memory_space=pltpu.VMEM)] * 7,
            out_specs=pl.BlockSpec(memory_space=pltpu.VMEM),
            scratch_shapes=scratch,
            compiler_params=pltpu.CompilerParams(
                collective_id=0, has_side_effects=True, vmem_limit_bytes=60 * 1024 * 1024),
        )(x, gain.reshape(1, -1), nbias.reshape(1, -1), up, ubias.reshape(1, -1), down,
          dbias.reshape(1, -1))

    return jax.shard_map(
        on_device,
        mesh=mesh,
        in_specs=(P(("img", "tp"), None), P(), P(), P("img", "tp"), P("tp"), P("tp", "img"), P()),
        out_specs=P(("img", "tp"), None),
        check_vma=False,
    )
```
